32 devices in a mesh: data: 1 (over z), pp: 4 (over y), ep: 8 (over x, core).
Axes of the slice: x: 4, y: 4, z: 1, core: 2. Of those that a mesh axis runs over, the one named last changes fastest.
The devices are a block of a 4x4x8 slice.
Arguments:
- expert_out: bfloat16 [4, 1, 256, 64, 4096], P('pp', 'data', 'ep')
- expert_ids: int32 [4, 1, 8, 128, 8], P('pp', 'data', 'ep')
- slot_ids: int32 [4, 1, 8, 128, 8], P('pp', 'data', 'ep')
- gate_weights: float32 [4, 1, 8, 128, 8], P('pp', 'data', 'ep')
- residual: bfloat16 [4, 1, 8, 128, 4096], P('pp', 'data', 'ep')
- norm_moe: float32 [4, 4096], P('pp')
- w_gate: bfloat16 [4, 4096, 1024], P('pp')
- w_up: bfloat16 [4, 4096, 1024], P('pp')
- w_down: bfloat16 [4, 1024, 4096], P('pp')
- norm_attn: float32 [4, 4096], P('pp')
- w_query: bfloat16 [4, 4096, 32, 128], P('pp')
- w_key: bfloat16 [4, 4096, 32, 128], P('pp')
- w_value: bfloat16 [4, 4096, 32, 128], P('pp')
- w_out: bfloat16 [4, 32, 128, 4096], P('pp')
Outputs:
- output: bfloat16 [4, 1, 8, 128, 4096], P('pp', 'data', 'ep')
All inputs are finite; a program needn't handle non-finite values.
Results may differ from the reference program's by a relative error of at most 0.0160459.
Values are sent between devices in bfloat16 or wider.
A program may use at most 768 MiB of HBM per device.

```python
import math
import jax
import jax.numpy as jnp
from jax import lax

STAGES = 4
EP_SIZE = 8
MICRO_BATCHES = 1
SEQ_DEV = 1
SEQ_LEN = 128
D_MODEL = 4096
NUM_HEADS = 32
HEAD_DIM = 128
EXPERTS = 256
TOP_K = 8
FF_SHARED = 1024
CAP_SLOTS = 8

SEQS = EP_SIZE * SEQ_DEV
TOK_DEV = SEQ_DEV * SEQ_LEN
TOKENS = SEQS * SEQ_LEN
SLOTS = EP_SIZE * CAP_SLOTS
HEADS_WIDTH = NUM_HEADS * HEAD_DIM
SCORE_SCALE = 1.0 / math.sqrt(HEAD_DIM)
EPSILON = 1e-6


def route_group(group_args):
    group_key, hot_draw = group_args
    hot_rank = jnp.argsort(jnp.argsort(hot_draw * EXPERTS + jnp.arange(EXPERTS)))
    lead_mask = (jnp.arange(TOK_DEV) <= CAP_SLOTS).astype(jnp.int32)[:, None]
    hot_bias = jnp.where(hot_rank < max(1, TOP_K // 4), 1024, 0) + jnp.where(hot_rank == 0, 8192, 0) * lead_mask
    noise_draw = jax.random.randint(group_key, (EP_SIZE, TOK_DEV, EXPERTS), 0, 4096)
    scores = (noise_draw + hot_bias) * EXPERTS + jnp.arange(EXPERTS)
    top_vals, expert_ids = lax.top_k(scores, TOP_K)
    choice_count = TOK_DEV * TOP_K
    flat_ids = expert_ids.reshape(EP_SIZE, choice_count)
    position = jnp.arange(choice_count)
    sort_order = jnp.argsort(flat_ids * choice_count + position, axis=-1)
    sorted_ids = jnp.take_along_axis(flat_ids, sort_order, axis=-1)
    is_start = jnp.concatenate([jnp.ones((EP_SIZE, 1), jnp.bool_), sorted_ids[:, 1:] != sorted_ids[:, :-1]], axis=1)
    start_pos = lax.cummax(jnp.where(is_start, position, 0), axis=1)
    slot_rank = jnp.take_along_axis(position - start_pos, jnp.argsort(sort_order, axis=-1), axis=-1)
    source = jnp.arange(EP_SIZE)[:, None]
    slot_ids = jnp.where(slot_rank < CAP_SLOTS, source * CAP_SLOTS + slot_rank, -1)
    return expert_ids.reshape(SEQS, SEQ_LEN, TOP_K), slot_ids.reshape(SEQS, SEQ_LEN, TOP_K)


def draw_routing(key):
    key_hot, key_score = jax.random.split(key)
    hot_draw = jax.random.randint(key_hot, (STAGES * MICRO_BATCHES, EXPERTS), 0, 1 << 20)
    group_keys = jax.random.split(key_score, STAGES * MICRO_BATCHES)
    expert_ids, slot_ids = lax.map(route_group, (group_keys, hot_draw))
    route_shape = (STAGES, MICRO_BATCHES, SEQS, SEQ_LEN, TOP_K)
    return expert_ids.reshape(route_shape), slot_ids.reshape(route_shape)


def setup_inputs(seed: int = 0, part: int = 0) -> dict:
    base_key = jax.random.key(seed)
    part_keys = jax.random.split(jax.random.fold_in(base_key, part), 5)
    expert_ids, slot_ids = draw_routing(part_keys[0])
    route_shape = (STAGES, MICRO_BATCHES, SEQS, SEQ_LEN, TOP_K)
    gate_draw = jax.random.normal(part_keys[1], route_shape, jnp.float32)
    gate_weights = jnp.exp(1.2 * gate_draw - 0.72) / TOP_K
    expert_scale = jax.random.uniform(part_keys[2], (STAGES * MICRO_BATCHES, EXPERTS, 1, 1), jnp.float32, 0.5, 3.0)
    out_keys = jax.random.split(part_keys[3], STAGES * MICRO_BATCHES)

    def draw_outputs(group_args):
        group_key, group_scale = group_args
        normal_draw = jax.random.normal(group_key, (EXPERTS, SLOTS, D_MODEL), jnp.float32)
        return (normal_draw * group_scale).astype(jnp.bfloat16)

    expert_out = lax.map(draw_outputs, (out_keys, expert_scale)).reshape(STAGES, MICRO_BATCHES, EXPERTS, SLOTS, D_MODEL)
    residual = jax.random.normal(part_keys[4], (STAGES, MICRO_BATCHES, SEQS, SEQ_LEN, D_MODEL), jnp.float32).astype(jnp.bfloat16)
    weight_keys = jax.random.split(jax.random.key(seed + 1), 9)
    in_scale = 1.0 / math.sqrt(D_MODEL)
    down_scale = 2.0 / math.sqrt(FF_SHARED)
    query_scale = 1.5 / math.sqrt(D_MODEL)
    out_scale = math.sqrt(math.sqrt(SEQ_LEN)) / math.sqrt(HEADS_WIDTH)
    norm_moe = jax.random.uniform(weight_keys[0], (STAGES, D_MODEL), jnp.float32, 0.5, 1.5)
    w_gate = (jax.random.normal(weight_keys[1], (STAGES, D_MODEL, FF_SHARED), jnp.float32) * in_scale).astype(jnp.bfloat16)
    w_up = (jax.random.normal(weight_keys[2], (STAGES, D_MODEL, FF_SHARED), jnp.float32) * in_scale).astype(jnp.bfloat16)
    w_down = (jax.random.normal(weight_keys[3], (STAGES, FF_SHARED, D_MODEL), jnp.float32) * down_scale).astype(jnp.bfloat16)
    norm_attn = jax.random.uniform(weight_keys[4], (STAGES, D_MODEL), jnp.float32, 0.5, 1.5)
    w_query = (jax.random.normal(weight_keys[5], (STAGES, D_MODEL, NUM_HEADS, HEAD_DIM), jnp.float32) * query_scale).astype(jnp.bfloat16)
    w_key = (jax.random.normal(weight_keys[6], (STAGES, D_MODEL, NUM_HEADS, HEAD_DIM), jnp.float32) * in_scale).astype(jnp.bfloat16)
    w_value = (jax.random.normal(weight_keys[7], (STAGES, D_MODEL, NUM_HEADS, HEAD_DIM), jnp.float32) * in_scale).astype(jnp.bfloat16)
    w_out = (jax.random.normal(weight_keys[8], (STAGES, NUM_HEADS, HEAD_DIM, D_MODEL), jnp.float32) * out_scale).astype(jnp.bfloat16)
    return {"expert_out": expert_out, "expert_ids": expert_ids, "slot_ids": slot_ids, "gate_weights": gate_weights, "residual": residual, "norm_moe": norm_moe, "w_gate": w_gate, "w_up": w_up, "w_down": w_down, "norm_attn": norm_attn, "w_query": w_query, "w_key": w_key, "w_value": w_value, "w_out": w_out}


def rms_norm(tensor, gain):
    values = tensor.astype(jnp.float32)
    inv_rms = lax.rsqrt(jnp.mean(values * values, axis=-1, keepdims=True) + EPSILON)
    return values * inv_rms * gain


def shared_expert(residual, norm_moe, w_gate, w_up, w_down):
    normed = rms_norm(residual, norm_moe).astype(jnp.bfloat16)
    gate_act = jnp.dot(normed, w_gate, preferred_element_type=jnp.float32)
    up_act = jnp.dot(normed, w_up, preferred_element_type=jnp.float32)
    hidden = (jax.nn.silu(gate_act) * up_act).astype(jnp.bfloat16)
    return jnp.dot(hidden, w_down, preferred_element_type=jnp.float32).astype(jnp.bfloat16)


def combine_micro(micro_args, stage_weights):
    expert_out, expert_ids, slot_ids, gate_weights, residual = micro_args
    norm_moe, w_gate, w_up, w_down = stage_weights
    flat_slots = slot_ids.reshape(TOKENS, TOP_K)
    kept_mask = flat_slots >= 0
    row_ids = expert_ids.reshape(TOKENS, TOP_K) * SLOTS + jnp.where(kept_mask, flat_slots, 0)
    picked = jnp.take(expert_out.reshape(EXPERTS * SLOTS, D_MODEL), row_ids, axis=0)
    weights = jnp.where(kept_mask, gate_weights.reshape(TOKENS, TOP_K), 0.0)
    routed = jnp.sum(picked.astype(jnp.float32) * weights[:, :, None], axis=1)
    flat_resid = residual.reshape(TOKENS, D_MODEL)
    shared = shared_expert(flat_resid, norm_moe, w_gate, w_up, w_down)
    combined = flat_resid.astype(jnp.float32) + shared.astype(jnp.float32) + routed
    return combined.astype(jnp.bfloat16).reshape(SEQS, SEQ_LEN, D_MODEL)


def attend_sequence(seq_args):
    queries, key_heads, value_heads = seq_args
    scores = jnp.einsum("qhe,khe->hqk", queries.astype(jnp.float32), key_heads.astype(jnp.float32)) * SCORE_SCALE
    causal = jnp.arange(SEQ_LEN)[:, None] >= jnp.arange(SEQ_LEN)[None, :]
    scores = jnp.where(causal, scores, -1e30)
    attn_probs = jnp.exp(scores - jnp.max(scores, axis=-1, keepdims=True))
    prob_sum = jnp.sum(attn_probs, axis=-1, keepdims=True)
    attn_mixed = jnp.einsum("hqk,khe->hqe", attn_probs.astype(jnp.bfloat16).astype(jnp.float32), value_heads.astype(jnp.float32))
    return attn_mixed / prob_sum


def attention_stage(stage_args):
    received, norm_attn, w_query, w_key, w_value, w_out = stage_args
    seq_count = MICRO_BATCHES * SEQS
    normed = rms_norm(received, norm_attn).astype(jnp.bfloat16).reshape(seq_count * SEQ_LEN, D_MODEL)

    def project(weight):
        product = jnp.dot(normed, weight.reshape(D_MODEL, HEADS_WIDTH), preferred_element_type=jnp.float32)
        return product.astype(jnp.bfloat16).reshape(seq_count, SEQ_LEN, NUM_HEADS, HEAD_DIM)

    attn_mixed = lax.map(attend_sequence, (project(w_query), project(w_key), project(w_value)))
    mixed_rows = jnp.transpose(attn_mixed.astype(jnp.bfloat16), (0, 2, 1, 3)).reshape(seq_count * SEQ_LEN, HEADS_WIDTH)
    attn_proj = jnp.dot(mixed_rows, w_out.reshape(HEADS_WIDTH, D_MODEL), preferred_element_type=jnp.float32).astype(jnp.bfloat16)
    updated = received.astype(jnp.float32) + attn_proj.astype(jnp.float32).reshape(received.shape)
    return updated.astype(jnp.bfloat16)


def reference(expert_out, expert_ids, slot_ids, gate_weights, residual, norm_moe, w_gate, w_up, w_down, norm_attn, w_query, w_key, w_value, w_out):
    def combine_stage(stage_args):
        def one_micro(micro_args):
            return combine_micro(micro_args, stage_args[5:])
        return lax.map(one_micro, stage_args[:5])

    combined = lax.map(combine_stage, (expert_out, expert_ids, slot_ids, gate_weights, residual, norm_moe, w_gate, w_up, w_down))
    received = jnp.roll(combined, 1, axis=0)
    return lax.map(attention_stage, (received, norm_attn, w_query, w_key, w_value, w_out))
```

```python
import functools
import math
import jax
import jax.numpy as jnp
from jax import lax
from jax.experimental import pallas as pl
from jax.experimental.pallas import tpu as pltpu
from jax.sharding import PartitionSpec as P

EPSILON = 1e-6
BF16 = jnp.bfloat16
F32 = jnp.float32
MESH = pl.DeviceIdType.MESH


def rms_norm(tensor, gain):
    values = tensor.astype(F32)
    inv_rms = lax.rsqrt(jnp.mean(values * values, axis=-1, keepdims=True) + EPSILON)
    return values * inv_rms * gain


def attention_block(combined, norm_attn, w_query, w_key, w_value, w_out):
    seq_len = combined.shape[1]
    score_scale = 1.0 / math.sqrt(w_query.shape[2])
    normed = rms_norm(combined, norm_attn).astype(BF16)
    queries = jnp.einsum("bld,dhe->blhe", normed, w_query, preferred_element_type=F32).astype(BF16)
    key_heads = jnp.einsum("bld,dhe->blhe", normed, w_key, preferred_element_type=F32).astype(BF16)
    value_heads = jnp.einsum("bld,dhe->blhe", normed, w_value, preferred_element_type=F32).astype(BF16)
    scores = jnp.einsum("bqhe,bkhe->bhqk", queries, key_heads, preferred_element_type=F32) * score_scale
    causal = jnp.arange(seq_len)[:, None] >= jnp.arange(seq_len)[None, :]
    scores = jnp.where(causal, scores, -1e30)
    attn_probs = jnp.exp(scores - jnp.max(scores, axis=-1, keepdims=True))
    prob_sum = jnp.sum(attn_probs, axis=-1, keepdims=True)
    attn_mixed = jnp.einsum("bhqk,bkhe->bhqe", attn_probs.astype(BF16), value_heads, preferred_element_type=F32) / prob_sum
    attn_proj = jnp.einsum("cirf,ife->cre", attn_mixed.astype(BF16), w_out, preferred_element_type=F32).astype(BF16)
    return (combined.astype(F32) + attn_proj.astype(F32)).astype(BF16)


def remote(src, dst, send, recv, where):
    return pltpu.make_async_remote_copy(src_ref=src, dst_ref=dst, send_sem=send, recv_sem=recv, device_id=where, device_id_type=MESH)


def combine_kernel(
    chunks, stages, chips,
    eo, ids, slots, gates, resid_hbm, gain, wg, wu, wd, yout,
    rows, part, relay, final, r_ids, r_slots, r_gates, resid, normed, gbuf, ubuf, dbuf, gacc, uacc, hidden, ysend, yin,
    s_load, s_rows, s_rowx, s_route, r_route, s_msg, r_msg, s_y, r_y, s_g, s_u, s_d,
):
    toks, dim = resid.shape
    half = dim // 2
    local_experts, cap = rows.shape[2], rows.shape[3]
    depth = 2 * local_experts * cap
    step_toks = toks // chunks
    me = lax.axis_index("ep")
    stage = lax.axis_index("pp")
    chip, core = lax.div(me, 2), lax.rem(me, 2)
    other = 1 - core

    def at_chip(offset, core_idx):
        return 2 * lax.rem(chip + offset, chips) + core_idx

    right, left, across, partner = at_chip(1, core), at_chip(chips - 1, core), at_chip(2, core), at_chip(0, other)
    nxt, prv = lax.rem(stage + 1, stages), lax.rem(stage + stages - 1, stages)

    order = (2, 1, 3, 0)
    own_loads = {}
    for k in order:
        own_loads[k] = pltpu.make_async_copy(eo.at[:, at_chip(k, core)], rows.at[k, core], s_load.at[k])
        own_loads[k].start()
    resid_load = pltpu.make_async_copy(resid_hbm, resid, s_load.at[4])
    resid_load.start()

    barrier = pltpu.get_barrier_semaphore()
    for peer in ({"ep": right}, {"ep": left}, {"ep": across}, {"ep": partner}, {"pp": nxt}, {"pp": prv}):
        pl.semaphore_signal(barrier, inc=1, device_id=peer, device_id_type=MESH)
    pl.semaphore_wait(barrier, 6)

    routing = []
    for offset in (2, 1, 3):
        slot = (chips - offset) % chips
        for n, (src, dst) in enumerate(((ids, r_ids), (slots, r_slots), (gates, r_gates))):
            copy = remote(src, dst.at[slot], s_route.at[offset, n], r_route.at[slot, n], {"ep": at_chip(offset, core)})
            copy.start()
            routing.append((slot, copy))
    row_sends = {}
    for k in order:
        row_sends[k] = remote(eo.at[:, at_chip(k, other)], rows.at[k, core], s_rows.at[k], s_rowx.at[k], {"ep": partner})
        row_sends[k].start()

    kstep = gbuf.shape[1]
    ksteps = dim // kstep
    nstep = dbuf.shape[2]
    nsteps = dim // nstep
    nbuf = gbuf.shape[0]

    def load_gu(i, slot):
        return (pltpu.make_async_copy(wg.at[pl.ds(i * kstep, kstep)], gbuf.at[slot], s_g.at[slot]),
                pltpu.make_async_copy(wu.at[pl.ds(i * kstep, kstep)], ubuf.at[slot], s_u.at[slot]))

    def load_d(i, slot):
        return pltpu.make_async_copy(wd.at[:, pl.ds(i * nstep, nstep)], dbuf.at[slot], s_d.at[slot])

    resid_load.wait()
    blk = 16

    def norm_rows(i, carry):
        at = pl.ds(pl.multiple_of(i * blk, blk), blk)
        values = resid[at, :].astype(F32)
        inv = lax.rsqrt(jnp.mean(values * values, axis=-1, keepdims=True) + EPSILON)
        normed[at, :] = (values * inv * gain[...]).astype(BF16)
        return carry

    lax.fori_loop(0, toks // blk, norm_rows, 0)

    ncol = min(512, dim)

    def partial_sum(k):
        dst = at_chip(k, core)
        if k == 0:
            e, s, g = ids[...], slots[...], gates[...]
        else:
            e, s, g = r_ids[k], r_slots[k], r_gates[k]
        where_row = jnp.where(s >= 0, (e - chip * (2 * local_experts)) * cap + s - dst * cap, -1)
        row_iota = lax.broadcasted_iota(jnp.int32, (depth, toks), 0)
        weight = jnp.zeros((depth, toks), F32)
        for j in range(e.shape[0]):
            weight = jnp.where(row_iota == where_row[j:j + 1, :], g[j:j + 1, :], weight)
        weight = weight.T
        high = weight.astype(BF16)
        rest = weight - high.astype(F32)
        mid = rest.astype(BF16)
        low = (rest - mid.astype(F32)).astype(BF16)

        def column(n, carry):
            at = pl.ds(pl.multiple_of(n * ncol, ncol), ncol)
            block = rows[k, :, :, :, at].reshape(depth, ncol)
            total = jnp.dot(high, block, preferred_element_type=F32)
            total += jnp.dot(mid, block, preferred_element_type=F32)
            total += jnp.dot(low, block, preferred_element_type=F32)
            part[k, :, at] = total
            return carry

        lax.fori_loop(0, dim // ncol, column, 0)

    lo, hi = pl.ds(0, half), pl.ds(half, half)

    def message(kind, t):
        tk = pl.ds(t * step_toks, step_toks)
        src, dst, dev = {
            0: (part.at[2, tk, lo], relay.at[0, tk], right),
            1: (part.at[2, tk, hi], relay.at[1, tk], left),
            2: (part.at[1, tk, hi], final.at[0, tk, hi], right),
            3: (part.at[3, tk, lo], final.at[1, tk, lo], left),
            4: (relay.at[0, tk], final.at[0, tk, lo], right),
            5: (relay.at[1, tk], final.at[1, tk, hi], left),
        }[kind]
        return remote(src, dst, s_msg.at[kind, t], r_msg.at[kind, t], {"ep": dev})

    def send(kind, t):
        if t < chunks:
            message(kind, t).start()

    def arrive(k):
        for slot, copy in routing:
            if slot == k:
                copy.wait_recv()
        own_loads[k].wait()
        row_sends[k].wait_recv()

    arrive(2)
    partial_sum(2)
    send(0, 0)
    send(1, 0)
    arrive(1)
    partial_sum(1)
    send(2, 0)
    send(0, 1)
    arrive(3)
    partial_sum(3)
    send(3, 0)
    send(1, 1)
    for slot in range(nbuf):
        for copy in load_gu(slot, slot):
            copy.start()
        load_d(slot, slot).start()
    own_loads[0].wait()
    row_sends[0].wait_recv()
    partial_sum(0)

    gacc[...] = jnp.zeros_like(gacc)
    uacc[...] = jnp.zeros_like(uacc)

    def gate_up(i, carry):
        slot = lax.rem(i, nbuf)
        for copy in load_gu(i, slot):
            copy.wait()
        xs = normed[:, pl.ds(pl.multiple_of(i * kstep, kstep), kstep)]
        gacc[...] += jnp.dot(xs, gbuf[slot], preferred_element_type=F32)
        uacc[...] += jnp.dot(xs, ubuf[slot], preferred_element_type=F32)

        @pl.when(i + nbuf < ksteps)
        def _():
            for copy in load_gu(i + nbuf, slot):
                copy.start()
        return carry

    lax.fori_loop(0, ksteps, gate_up, 0)
    gate_act = gacc[...]
    hidden[...] = (gate_act * jax.nn.sigmoid(gate_act) * uacc[...]).astype(BF16)

    def down(i, carry):
        slot = lax.rem(i, nbuf)
        load_d(i, slot).wait()
        at = pl.ds(pl.multiple_of(i * nstep, nstep), nstep)
        shared = jnp.dot(hidden[...], dbuf[slot], preferred_element_type=F32).astype(BF16)
        part[0, :, at] += resid[:, at].astype(F32) + shared.astype(F32)

        @pl.when(i + nbuf < nsteps)
        def _():
            load_d(i + nbuf, slot).start()
        return carry

    lax.fori_loop(0, nsteps, down, 0)

    def forward(t):
        tk = pl.ds(t * step_toks, step_toks)
        message(0, t).wait_recv()
        relay[0, tk, :] += part[1, tk, lo]
        send(4, t)
        message(1, t).wait_recv()
        relay[1, tk, :] += part[3, tk, hi]
        send(5, t)
        send(2, t + 1)
        send(3, t + 1)
        send(0, t + 2)
        send(1, t + 2)

    def shift(t):
        tk = pl.ds(t * step_toks, step_toks)
        return remote(ysend.at[tk], yin.at[tk], s_y.at[t], r_y.at[t], {"pp": nxt})

    def finish(t):
        tk = pl.ds(t * step_toks, step_toks)
        for kind in (2, 3, 4, 5):
            message(kind, t).wait_recv()
        ysend[tk, :] = (part[0, tk, :] + final[0, tk, :] + final[1, tk, :]).astype(BF16)
        shift(t).start()

    for t in range(chunks):
        forward(t)
        if t > 0:
            finish(t - 1)
    finish(chunks - 1)

    for t in range(chunks):
        shift(t).wait_recv()
    out_copy = pltpu.make_async_copy(yin, yout, s_load.at[5])
    out_copy.start()
    for slot, copy in routing:
        copy.wait_send()
    for k in order:
        row_sends[k].wait_send()
    for t in range(chunks):
        for kind in range(6):
            message(kind, t).wait_send()
        shift(t).wait_send()
    out_copy.wait()


def combine(stages, chips, eo, ids, slots, gates, resid, gain, wg, wu, wd):
    local_experts, owners, cap, dim = eo.shape
    toks = resid.shape[0]
    ff = wg.shape[1]
    chunks = 4
    nbuf = 2
    kstep, nstep = min(512, dim // nbuf), min(512, dim // nbuf)
    top_k = ids.shape[0]
    any_spec = pl.BlockSpec(memory_space=pl.ANY)
    vmem = pl.BlockSpec(memory_space=pltpu.VMEM)
    dma = pltpu.SemaphoreType.DMA
    scratch = [
        pltpu.VMEM((chips, 2, local_experts, cap, dim), BF16),
        pltpu.VMEM((chips, toks, dim), F32),
        pltpu.VMEM((2, toks, dim // 2), F32),
        pltpu.VMEM((2, toks, dim), F32),
        pltpu.VMEM((chips, top_k, toks), jnp.int32),
        pltpu.VMEM((chips, top_k, toks), jnp.int32),
        pltpu.VMEM((chips, top_k, toks), F32),
        pltpu.VMEM((toks, dim), BF16),
        pltpu.VMEM((toks, dim), BF16),
        pltpu.VMEM((nbuf, kstep, ff), BF16),
        pltpu.VMEM((nbuf, kstep, ff), BF16),
        pltpu.VMEM((nbuf, ff, nstep), BF16),
        pltpu.VMEM((toks, ff), F32),
        pltpu.VMEM((toks, ff), F32),
        pltpu.VMEM((toks, ff), BF16),
        pltpu.VMEM((toks, dim), BF16),
        pltpu.VMEM((toks, dim), BF16),
        dma((6,)), dma((chips,)), dma((chips,)), dma((chips, 3)), dma((chips, 3)),
        dma((6, chunks)), dma((6, chunks)), dma((chunks,)), dma((chunks,)),
        dma((nbuf,)), dma((nbuf,)), dma((nbuf,)),
    ]
    return pl.pallas_call(
        functools.partial(combine_kernel, chunks, stages, chips),
        out_shape=jax.ShapeDtypeStruct((toks, dim), BF16),
        in_specs=[any_spec, vmem, vmem, vmem, any_spec, vmem, any_spec, any_spec, any_spec],
        out_specs=any_spec,
        scratch_shapes=scratch,
        cost_estimate=pl.CostEstimate(flops=20_000_000_000, bytes_accessed=50_000_000, transcendentals=0),
        compiler_params=pltpu.CompilerParams(collective_id=0, has_side_effects=True, vmem_limit_bytes=60 * 2**20),
        name="combine",
    )(eo, ids, slots, gates, resid, gain, wg, wu, wd)


def solution(mesh):
    stages = mesh.shape["pp"]
    ep_size = mesh.shape["ep"]
    tok_spec = P("pp", "data", "ep", None, None)
    vec_spec = P("pp", None)
    mat_spec = P("pp", None, None)
    head_spec = P("pp", None, None, None)

    def device_step(expert_out, expert_ids, slot_ids, gate_weights, residual, norm_moe, w_gate, w_up, w_down, norm_attn, w_query, w_key, w_value, w_out):
        local_experts, slots_total, model_dim = expert_out.shape[2:]
        cap = slots_total // ep_size
        eo = expert_out[0, 0].reshape(local_experts, ep_size, cap, model_dim)
        toks = residual.shape[3]

        def flip(array):
            return jnp.swapaxes(array[0, 0].reshape(toks, -1), 0, 1)

        incoming = combine(stages, ep_size // 2, eo, flip(expert_ids), flip(slot_ids), flip(gate_weights),
                           residual[0, 0, 0], norm_moe, w_gate[0], w_up[0], w_down[0])
        out = attention_block(incoming[None], norm_attn[0], w_query[0], w_key[0], w_value[0], w_out[0])
        return out[None, None]

    in_specs = (tok_spec,) * 5 + (vec_spec, mat_spec, mat_spec, mat_spec, vec_spec, head_spec, head_spec, head_spec, head_spec)
    return jax.shard_map(device_step, mesh=mesh, in_specs=in_specs, out_specs=tok_spec, check_vma=False)
```

```python
import functools
import math
import jax
import jax.numpy as jnp
from jax import lax
from jax.experimental import pallas as pl
from jax.experimental.pallas import tpu as pltpu
from jax.sharding import PartitionSpec as P

EPSILON = 1e-6
BF16 = jnp.bfloat16
F32 = jnp.float32
MESH = pl.DeviceIdType.MESH


def remote(src, dst, send, recv, where):
    return pltpu.make_async_remote_copy(src_ref=src, dst_ref=dst, send_sem=send, recv_sem=recv, device_id=where, device_id_type=MESH)


def stage_kernel(
    chunks, stages, chips,
    eo, ids, slots, gates, resid_hbm, gain_moe, gain_attn, wg, wu, wd, wq, wk, wv, wo, out_hbm,
    pool, nat, part, relay, final, r_ids, r_slots, r_gates, resid, normed, hidden, ysend, yin, kbuf,
    s_load, s_pool, s_nat, s_rows, s_rowx, s_route, r_route, s_msg, r_msg, s_y, r_y,
):
    toks, dim = resid.shape
    half = dim // 2
    groups = pool.shape[1]
    local_experts = groups // 2
    cap = pool.shape[2]
    depth = groups * cap
    step_toks = toks // chunks
    head_dim = nat.shape[3]
    half_heads = nat.shape[2]
    ksteps = dim // depth
    slabs = 2 * ksteps
    ff = wg.shape[2]
    fsteps = ff // depth
    nat_slots = nat.shape[0]
    me = lax.axis_index("ep")
    stage = lax.axis_index("pp")
    chip, core = lax.div(me, 2), lax.rem(me, 2)
    other = 1 - core

    def at_chip(offset, core_idx):
        return 2 * lax.rem(chip + offset, chips) + core_idx

    right, left, across, partner = at_chip(1, core), at_chip(chips - 1, core), at_chip(2, core), at_chip(0, other)
    nxt, prv = lax.rem(stage + 1, stages), lax.rem(stage + stages - 1, stages)
    order = (2, 1, 3, 0)
    halves = (pl.ds(0, half), pl.ds(half, half))
    lo, hi = halves

    own_loads = {}
    for k in order:
        own_loads[k] = [pltpu.make_async_copy(eo.at[:, at_chip(k, core), :, halves[h]],
                                              pool.at[2 * k + h, pl.ds(core * local_experts, local_experts)], s_load.at[2 * k + h])
                        for h in range(2)]
    for copy in own_loads[2]:
        copy.start()
    resid_load = pltpu.make_async_copy(resid_hbm, resid, s_load.at[2 * chips])
    resid_load.start()

    barrier = pltpu.get_barrier_semaphore()
    for peer in ({"ep": right}, {"ep": left}, {"ep": across}, {"ep": partner}, {"pp": nxt}, {"pp": prv}):
        pl.semaphore_signal(barrier, inc=1, device_id=peer, device_id_type=MESH)
    pl.semaphore_wait(barrier, 6)

    routing = []
    for offset in (2, 1, 3):
        slot = (chips - offset) % chips
        for n, (src, dst) in enumerate(((ids, r_ids), (slots, r_slots), (gates, r_gates))):
            copy = remote(src, dst.at[slot], s_route.at[offset, n], r_route.at[slot, n], {"ep": at_chip(offset, core)})
            copy.start()
            routing.append((slot, copy))
    row_sends = {}
    for k in order:
        row_sends[k] = [remote(eo.at[:, at_chip(k, other), :, halves[h]],
                               pool.at[2 * k + h, pl.ds(core * local_experts, local_experts)],
                               s_rows.at[2 * k + h], s_rowx.at[2 * k + h], {"ep": partner})
                        for h in range(2)]
    for copy in row_sends[2]:
        copy.start()
    for k in order[1:]:
        for copy in own_loads[k]:
            copy.start()

    first_shared = 2 * chips

    def load_gate_up(i):
        slot = first_shared + i
        at = pl.ds(i * groups, groups)
        return (pltpu.make_async_copy(wg.at[at], pool.at[slot, :, :, pl.ds(0, ff)], s_pool.at[0, slot]),
                pltpu.make_async_copy(wu.at[at], pool.at[slot, :, :, pl.ds(ff, ff)], s_pool.at[1, slot]))

    def load_rows(matrix, hh, i, slot):
        return pltpu.make_async_copy(matrix.at[pl.ds(i * groups, groups), :, pl.ds(pl.multiple_of(hh * half, half), half)],
                                     pool.at[slot], s_pool.at[0, slot])

    def load_heads(matrix, j, slot):
        hh, i = lax.div(j, ksteps), lax.rem(j, ksteps)
        return pltpu.make_async_copy(matrix.at[pl.ds(i * depth, depth), pl.ds(pl.multiple_of(hh * half_heads, half_heads), half_heads)],
                                     nat.at[slot], s_nat.at[slot])

    blk = min(16, step_toks)

    def norm_rows(src, gain, i):
        at = pl.ds(pl.multiple_of(i * blk, blk), blk)
        values = src[at, :].astype(F32)
        inv = lax.rsqrt(jnp.mean(values * values, axis=-1, keepdims=True) + EPSILON)
        normed[at, :] = (values * inv * gain[...]).astype(BF16)

    resid_load.wait()

    def norm_resid(i, carry):
        norm_rows(resid, gain_moe, i)
        return carry

    lax.fori_loop(0, toks // blk, norm_resid, 0)

    ncol = min(512, half)

    def partial_sum(k):
        dst = at_chip(k, core)
        if k == 0:
            e, s, g = ids[...], slots[...], gates[...]
        else:
            e, s, g = r_ids[k], r_slots[k], r_gates[k]
        where_row = jnp.where(s >= 0, (e - chip * (2 * local_experts)) * cap + s - dst * cap, -1)
        row_iota = lax.broadcasted_iota(jnp.int32, (depth, toks), 0)
        weight = jnp.zeros((depth, toks), F32)
        for j in range(e.shape[0]):
            weight = jnp.where(row_iota == where_row[j:j + 1, :], g[j:j + 1, :], weight)
        weight = weight.T
        high = weight.astype(BF16)
        rest = weight - high.astype(F32)
        mid = rest.astype(BF16)
        low = (rest - mid.astype(F32)).astype(BF16)
        for h in range(2):
            def column(n, carry):
                start = pl.multiple_of(n * ncol, ncol)
                block = pool[2 * k + h, :, :, pl.ds(start, ncol)].reshape(depth, ncol)
                total = jnp.dot(high, block, preferred_element_type=F32)
                total += jnp.dot(mid, block, preferred_element_type=F32)
                total += jnp.dot(low, block, preferred_element_type=F32)
                part[k, :, pl.ds(pl.multiple_of(h * half + start, ncol), ncol)] = total
                return carry

            lax.fori_loop(0, half // ncol, column, 0)

    def message(kind, t):
        tk = pl.ds(t * step_toks, step_toks)
        src, dst, dev = {
            0: (part.at[2, tk, lo], relay.at[0, tk], right),
            1: (part.at[2, tk, hi], relay.at[1, tk], left),
            2: (part.at[1, tk, hi], final.at[0, tk, hi], right),
            3: (part.at[3, tk, lo], final.at[1, tk, lo], left),
            4: (relay.at[0, tk], final.at[0, tk, lo], right),
            5: (relay.at[1, tk], final.at[1, tk, hi], left),
        }[kind]
        return remote(src, dst, s_msg.at[kind, t], r_msg.at[kind, t], {"ep": dev})

    def send(kind, t):
        if t < chunks:
            message(kind, t).start()

    def arrive(k, following):
        for slot, copy in routing:
            if slot == k:
                copy.wait_recv()
        for copy in own_loads[k]:
            copy.wait()
        for copy in row_sends[k]:
            copy.wait_recv()
        if following is not None:
            for copy in row_sends[following]:
                copy.start()

    ahead = min(3, chunks)
    arrive(2, 1)
    for i in range(ksteps):
        for copy in load_gate_up(i):
            copy.start()
    partial_sum(2)
    for t in range(ahead):
        send(0, t)
        send(1, t)
    arrive(1, 3)
    partial_sum(1)
    send(2, 0)
    arrive(3, 0)
    partial_sum(3)
    send(3, 0)
    for n in range(2 * fsteps):
        load_rows(wd, n // fsteps, n % fsteps, 4 + n).start()

    for i in range(ksteps):
        for copy in load_gate_up(i):
            copy.wait()
        product = jnp.dot(normed[:, i * depth:(i + 1) * depth], pool[first_shared + i].reshape(depth, half), preferred_element_type=F32)
        part[0, :, lo] = product if i == 0 else part[0, :, lo] + product
    gate_act = part[0, :, pl.ds(0, ff)]
    hidden[...] = (gate_act * jax.nn.sigmoid(gate_act) * part[0, :, pl.ds(ff, ff)]).astype(BF16)
    arrive(0, None)
    partial_sum(0)
    for hh in range(2):
        for i in range(fsteps):
            load_rows(wd, hh, i, 4 + hh * fsteps + i).wait()
        for n in range(half // ncol):
            at = pl.ds(hh * half + n * ncol, ncol)
            product = None
            for i in range(fsteps):
                block = pool[4 + hh * fsteps + i, :, :, pl.ds(n * ncol, ncol)].reshape(depth, ncol)
                term = jnp.dot(hidden[:, i * depth:(i + 1) * depth], block, preferred_element_type=F32)
                product = term if product is None else product + term
            part[0, :, at] += resid[:, at].astype(F32) + product.astype(BF16).astype(F32)

    def forward(t):
        tk = pl.ds(t * step_toks, step_toks)
        message(0, t).wait_recv()
        relay[0, tk, :] += part[1, tk, lo]
        send(4, t)
        message(1, t).wait_recv()
        relay[1, tk, :] += part[3, tk, hi]
        send(5, t)
        send(2, t + 1)
        send(3, t + 1)
        send(0, t + ahead)
        send(1, t + ahead)

    def shift(t):
        tk = pl.ds(t * step_toks, step_toks)
        return remote(ysend.at[tk], yin.at[tk], s_y.at[t], r_y.at[t], {"pp": nxt})

    def finish(t):
        tk = pl.ds(t * step_toks, step_toks)
        for kind in (2, 3, 4, 5):
            message(kind, t).wait_recv()
        ysend[tk, :] = (part[0, tk, :] + final[0, tk, :] + final[1, tk, :]).astype(BF16)
        shift(t).start()

    def receive(t):
        shift(t).wait_recv()
        for i in range(step_toks // blk):
            norm_rows(yin, gain_attn, t * (step_toks // blk) + i)

    for slot in range(nat_slots):
        load_heads(wq, slot, slot).start()

    def lay_out(j, carry):
        slot = lax.rem(j, nat_slots)
        load_heads(wq, j, slot).wait()
        pool[j] = nat[slot].reshape(groups, cap, half)

        @pl.when(j + nat_slots < slabs)
        def _():
            load_heads(wq, j + nat_slots, slot).start()

        @pl.when(j + nat_slots >= slabs)
        def _():
            load_heads(wk, j + nat_slots - slabs, slot).start()
        return carry

    per_chunk = -(-slabs // max(1, chunks - 2))
    done = 0
    for t in range(chunks):
        forward(t)
        if t > 0:
            finish(t - 1)
        if t > 1:
            receive(t - 2)
        upto = min(slabs, done + per_chunk) if t < chunks - 1 else slabs
        if upto > done:
            lax.fori_loop(done, upto, lay_out, 0)
        done = upto
    if chunks > 1:
        receive(chunks - 2)
    finish(chunks - 1)
    for t in range(chunks):
        for kind in range(6):
            message(kind, t).wait_send()
    part[1] = jnp.zeros((toks, dim), F32)
    part[2] = jnp.zeros((toks, dim), F32)
    part[3] = jnp.zeros((toks, dim), F32)
    receive(chunks - 1)

    qbuf, vbuf = resid, ysend

    def query(i, carry):
        for hh in range(2):
            at = halves[hh]
            product = jnp.dot(normed[:, pl.ds(pl.multiple_of(i * depth, depth), depth)], pool[hh * ksteps + i].reshape(depth, half), preferred_element_type=F32)
            part[1, :, at] += product
        load_rows(wo, 0, i, i).start()
        return carry

    lax.fori_loop(0, ksteps, query, 0)
    qbuf[...] = part[1].astype(BF16)

    def slot_of(index):
        return lax.rem(index, nat_slots)

    def stream(which, matrix, following):
        for hh in range(2):
            at = halves[hh]

            def step(i, carry):
                j = hh * ksteps + i
                slot = slot_of(j + (1 + which) * slabs)
                load_heads(matrix, j, slot).wait()
                part[2 + which, :, at] += jnp.dot(normed[:, pl.ds(pl.multiple_of(i * depth, depth), depth)], nat[slot].reshape(depth, half), preferred_element_type=F32)
                nj = j + nat_slots

                @pl.when(nj < slabs)
                def _():
                    load_heads(matrix, nj, slot).start()

                if following is not None:
                    @pl.when(nj >= slabs)
                    def _():
                        load_heads(following, nj - slabs, slot).start()

                if which == 0 and hh == 0:
                    load_rows(wo, 1, i, ksteps + i).start()
                return carry

            lax.fori_loop(0, ksteps, step, 0)

    stream(0, wk, wv)
    kbuf[...] = part[2].astype(BF16)
    stream(1, wv, None)
    for t in range(chunks):
        shift(t).wait_send()
    vbuf[...] = part[3].astype(BF16)

    scale = 1.0 / math.sqrt(head_dim)
    causal = lax.broadcasted_iota(jnp.int32, (toks, toks), 0) >= lax.broadcasted_iota(jnp.int32, (toks, toks), 1)
    together = 4

    def heads(n, carry):
        cols = [pl.ds(pl.multiple_of((n * together + m) * head_dim, head_dim), head_dim) for m in range(together)]
        scores = [lax.dot_general(qbuf[:, at], kbuf[:, at], (((1,), (1,)), ((), ())), preferred_element_type=F32) for at in cols]
        scores = [jnp.where(causal, s * scale, -1e30) for s in scores]
        probs = [jnp.exp(s - jnp.max(s, axis=-1, keepdims=True)) for s in scores]
        sums = [jnp.sum(p, axis=-1, keepdims=True) for p in probs]
        mixed = [jnp.dot(p.astype(BF16), vbuf[:, at], preferred_element_type=F32) for p, at in zip(probs, cols)]
        for at, value, total in zip(cols, mixed, sums):
            qbuf[:, at] = (value / total).astype(BF16)
        return carry

    lax.fori_loop(0, dim // (head_dim * together), heads, 0)

    out_copies = []
    for hh in range(2):
        at = halves[hh]
        for i in range(ksteps):
            load_rows(wo, hh, i, hh * ksteps + i).wait()
        for n in range(half // ncol):
            cols = pl.ds(hh * half + n * ncol, ncol)

            def proj(i, total):
                block = pool[hh * ksteps + i, :, :, pl.ds(n * ncol, ncol)].reshape(depth, ncol)
                return total + jnp.dot(qbuf[:, pl.ds(pl.multiple_of(i * depth, depth), depth)], block, preferred_element_type=F32)

            total = jnp.zeros((toks, ncol), F32)
            for i in range(ksteps):
                total = proj(i, total)
            kbuf[:, cols] = (yin[:, cols].astype(F32) + total.astype(BF16).astype(F32)).astype(BF16)
        copy = pltpu.make_async_copy(kbuf.at[:, at], out_hbm.at[:, at], s_load.at[hh])
        copy.start()
        out_copies.append(copy)

    for slot, copy in routing:
        copy.wait_send()
    for k in order:
        for copy in row_sends[k]:
            copy.wait_send()
    for copy in out_copies:
        copy.wait()


def run_stage(stages, chips, eo, ids, slots, gates, resid, gain_moe, gain_attn, wg, wu, wd, wq, wk, wv, wo):
    local_experts, owners, cap, dim = eo.shape
    toks = resid.shape[0]
    heads, head_dim = wq.shape[1:]
    ff = wg.shape[1]
    groups = 2 * local_experts
    depth = groups * cap
    half = dim // 2
    chunks = 8
    nat_slots = 4
    top_k = ids.shape[0]
    pool_slots = max(2 * dim // depth, 2 * chips + dim // depth)
    any_spec = pl.BlockSpec(memory_space=pl.ANY)
    vmem = pl.BlockSpec(memory_space=pltpu.VMEM)
    dma = pltpu.SemaphoreType.DMA
    scratch = [
        pltpu.VMEM((pool_slots, groups, cap, half), BF16),
        pltpu.VMEM((nat_slots, depth, heads // 2, head_dim), BF16),
        pltpu.VMEM((chips, toks, dim), F32),
        pltpu.VMEM((2, toks, half), F32),
        pltpu.VMEM((2, toks, dim), F32),
        pltpu.VMEM((chips, top_k, toks), jnp.int32),
        pltpu.VMEM((chips, top_k, toks), jnp.int32),
        pltpu.VMEM((chips, top_k, toks), F32),
        pltpu.VMEM((toks, dim), BF16),
        pltpu.VMEM((toks, dim), BF16),
        pltpu.VMEM((toks, ff), BF16),
        pltpu.VMEM((toks, dim), BF16),
        pltpu.VMEM((toks, dim), BF16),
        pltpu.VMEM((toks, dim), BF16),
        dma((2 * chips + 1,)), dma((2, pool_slots)), dma((nat_slots,)), dma((2 * chips,)), dma((2 * chips,)),
        dma((chips, 3)), dma((chips, 3)), dma((6, chunks)), dma((6, chunks)), dma((chunks,)), dma((chunks,)),
    ]

    def grouped(matrix):
        return matrix.reshape(-1, cap, matrix.shape[-1])

    return pl.pallas_call(
        functools.partial(stage_kernel, chunks, stages, chips),
        out_shape=jax.ShapeDtypeStruct((toks, dim), BF16),
        in_specs=[any_spec, vmem, vmem, vmem, any_spec, vmem, vmem] + [any_spec] * 7,
        out_specs=any_spec,
        scratch_shapes=scratch,
        cost_estimate=pl.CostEstimate(flops=40_000_000_000, bytes_accessed=180_000_000, transcendentals=0),
        compiler_params=pltpu.CompilerParams(collective_id=0, has_side_effects=True, vmem_limit_bytes=67_043_328),
        name="stage",
    )(eo, ids, slots, gates, resid, gain_moe, gain_attn, grouped(wg), grouped(wu), grouped(wd), wq, wk, wv, grouped(wo))


def solution(mesh):
    stages = mesh.shape["pp"]
    ep_size = mesh.shape["ep"]
    tok_spec = P("pp", "data", "ep", None, None)
    vec_spec = P("pp", None)
    mat_spec = P("pp", None, None)
    head_spec = P("pp", None, None, None)

    def device_step(expert_out, expert_ids, slot_ids, gate_weights, residual, norm_moe, w_gate, w_up, w_down, norm_attn, w_query, w_key, w_value, w_out):
        local_experts, slots_total, model_dim = expert_out.shape[2:]
        cap = slots_total // ep_size
        eo = expert_out[0, 0].reshape(local_experts, ep_size, cap, model_dim)
        toks = residual.shape[3]

        def flip(array):
            return jnp.swapaxes(array[0, 0].reshape(toks, -1), 0, 1)

        out = run_stage(stages, ep_size // 2, eo, flip(expert_ids), flip(slot_ids), flip(gate_weights), residual[0, 0, 0],
                        norm_moe, norm_attn, w_gate[0], w_up[0], w_down[0], w_query[0], w_key[0], w_value[0],
                        w_out[0].reshape(-1, model_dim))
        return out[None, None, None]

    in_specs = (tok_spec,) * 5 + (vec_spec, mat_spec, mat_spec, mat_spec, vec_spec, head_spec, head_spec, head_spec, head_spec)
    return jax.shard_map(device_step, mesh=mesh, in_specs=in_specs, out_specs=tok_spec, check_vma=False)
```

```python
import functools
import math
import jax
import jax.numpy as jnp
from jax import lax
from jax.experimental import pallas as pl
from jax.experimental.pallas import tpu as pltpu
from jax.sharding import PartitionSpec as P

EPSILON = 1e-6
BF16 = jnp.bfloat16
F32 = jnp.float32
MESH = pl.DeviceIdType.MESH


def remote(src, dst, send, recv, where):
    return pltpu.make_async_remote_copy(src_ref=src, dst_ref=dst, send_sem=send, recv_sem=recv, device_id=where, device_id_type=MESH)


def stage_kernel(
    chunks, stages, chips,
    eo, ids, slots, gates, resid_hbm, gain_moe_hbm, gain_attn_hbm, wg, wu, wd, wq, wk, wv, wo, out_hbm,
    pool, nat, part, relay, final, r_ids, r_slots, r_gates, gain_moe, gain_attn, resid, normed, hidden, ysend, yin, kbuf,
    s_load, s_pool, s_nat, s_rows, s_rowx, s_route, r_route, s_msg, r_msg, s_y, r_y,
):
    toks, dim = resid.shape
    half = dim // 2
    groups = pool.shape[1]
    local_experts = groups // 2
    cap = pool.shape[2]
    depth = groups * cap
    step_toks = toks // chunks
    head_dim = nat.shape[3]
    half_heads = nat.shape[2]
    ksteps = dim // depth
    slabs = 2 * ksteps
    ff = wg.shape[2]
    fsteps = ff // depth
    nat_slots = nat.shape[0]
    me = lax.axis_index("ep")
    stage = lax.axis_index("pp")
    chip, core = lax.div(me, 2), lax.rem(me, 2)
    other = 1 - core

    def at_chip(offset, core_idx):
        return 2 * lax.rem(chip + offset, chips) + core_idx

    right, left, across, partner = at_chip(1, core), at_chip(chips - 1, core), at_chip(2, core), at_chip(0, other)
    nxt, prv = lax.rem(stage + 1, stages), lax.rem(stage + stages - 1, stages)
    order = (2, 1, 3, 0)
    halves = (pl.ds(0, half), pl.ds(half, half))
    lo, hi = halves

    barrier = pltpu.get_barrier_semaphore()
    for peer in ({"ep": across}, {"ep": right}, {"ep": left}, {"ep": partner}, {"pp": nxt}, {"pp": prv}):
        pl.semaphore_signal(barrier, inc=1, device_id=peer, device_id_type=MESH)
    own_loads = {}
    for k in order:
        own_loads[k] = [pltpu.make_async_copy(eo.at[:, at_chip(k, core), :, halves[h]],
                                              pool.at[2 * k + h, pl.ds(core * local_experts, local_experts)], s_load.at[2 * k + h])
                        for h in range(2)]
    small = [(resid_hbm, resid), (gain_moe_hbm, gain_moe), (gain_attn_hbm, gain_attn),
             (ids, r_ids.at[0]), (slots, r_slots.at[0]), (gates, r_gates.at[0])]
    small_loads = [pltpu.make_async_copy(src, dst, s_load.at[2 * chips + n]) for n, (src, dst) in enumerate(small)]
    for copy in own_loads[2] + small_loads:
        copy.start()
    pl.semaphore_wait(barrier, 6)

    routing = []
    for offset in (2, 1, 3):
        slot = (chips - offset) % chips
        for n, (src, dst) in enumerate(((ids, r_ids), (slots, r_slots), (gates, r_gates))):
            copy = remote(src, dst.at[slot], s_route.at[offset, n], r_route.at[slot, n], {"ep": at_chip(offset, core)})
            copy.start()
            routing.append((slot, copy))
    row_sends = {}
    for k in order:
        row_sends[k] = [remote(eo.at[:, at_chip(k, other), :, halves[h]],
                               pool.at[2 * k + h, pl.ds(core * local_experts, local_experts)],
                               s_rows.at[2 * k + h], s_rowx.at[2 * k + h], {"ep": partner})
                        for h in range(2)]
    for copy in row_sends[2]:
        copy.start()
    for k in order[1:]:
        for copy in own_loads[k]:
            copy.start()

    first_shared = 2 * chips

    def load_gate_up(i):
        slot = first_shared + i
        at = pl.ds(i * groups, groups)
        return (pltpu.make_async_copy(wg.at[at], pool.at[slot, :, :, pl.ds(0, ff)], s_pool.at[0, slot]),
                pltpu.make_async_copy(wu.at[at], pool.at[slot, :, :, pl.ds(ff, ff)], s_pool.at[1, slot]))

    def load_rows(matrix, hh, i, slot):
        return pltpu.make_async_copy(matrix.at[pl.ds(i * groups, groups), :, pl.ds(pl.multiple_of(hh * half, half), half)],
                                     pool.at[slot], s_pool.at[0, slot])

    def load_heads(matrix, j, slot):
        hh, i = lax.div(j, ksteps), lax.rem(j, ksteps)
        return pltpu.make_async_copy(matrix.at[pl.ds(i * depth, depth), pl.ds(pl.multiple_of(hh * half_heads, half_heads), half_heads)],
                                     nat.at[slot], s_nat.at[slot])

    blk = min(16, step_toks)

    def norm_rows(src, gain, i):
        at = pl.ds(pl.multiple_of(i * blk, blk), blk)
        values = src[at, :].astype(F32)
        inv = lax.rsqrt(jnp.mean(values * values, axis=-1, keepdims=True) + EPSILON)
        normed[at, :] = (values * inv * gain[...]).astype(BF16)

    for copy in small_loads:
        copy.wait()

    def norm_resid(i, carry):
        norm_rows(resid, gain_moe, i)
        return carry

    lax.fori_loop(0, toks // blk, norm_resid, 0)

    ncol = min(512, half)

    def gate_matrix(k):
        dst = at_chip(k, core)
        e, s, g = r_ids[k], r_slots[k], r_gates[k]
        where_row = jnp.where(s >= 0, (e - chip * (2 * local_experts)) * cap + s - dst * cap, -1)
        row_iota = lax.broadcasted_iota(jnp.int32, (depth, toks), 0)
        weight = jnp.zeros((depth, toks), F32)
        for j in range(e.shape[0]):
            weight = jnp.where(row_iota == where_row[j:j + 1, :], g[j:j + 1, :], weight)
        weight = weight.T
        high = weight.astype(BF16)
        rest = weight - high.astype(F32)
        mid = rest.astype(BF16)
        low = (rest - mid.astype(F32)).astype(BF16)
        return high, mid, low

    def partial_sum(k, h, weights):
        def column(n, carry):
            start = pl.multiple_of(n * ncol, ncol)
            block = pool[2 * k + h, :, :, pl.ds(start, ncol)].reshape(depth, ncol)
            total = jnp.dot(weights[0], block, preferred_element_type=F32)
            total += jnp.dot(weights[1], block, preferred_element_type=F32)
            total += jnp.dot(weights[2], block, preferred_element_type=F32)
            part[k, :, pl.ds(pl.multiple_of(h * half + start, ncol), ncol)] = total
            return carry

        lax.fori_loop(0, half // ncol, column, 0)

    def message(kind, t):
        tk = pl.ds(t * step_toks, step_toks)
        src, dst, dev = {
            0: (part.at[2, tk, lo], relay.at[0, tk], right),
            1: (part.at[2, tk, hi], relay.at[1, tk], left),
            2: (part.at[1, tk, hi], final.at[0, tk, hi], right),
            3: (part.at[3, tk, lo], final.at[1, tk, lo], left),
            4: (relay.at[0, tk], final.at[0, tk, lo], right),
            5: (relay.at[1, tk], final.at[1, tk, hi], left),
        }[kind]
        return remote(src, dst, s_msg.at[kind, t], r_msg.at[kind, t], {"ep": dev})

    def send(kind, t):
        if t < chunks:
            message(kind, t).start()

    def routing_arrived(k):
        for slot, copy in routing:
            if slot == k:
                copy.wait_recv()

    def rows_arrived(k, h):
        own_loads[k][h].wait()
        row_sends[k][h].wait_recv()

    def start_rows(k):
        for copy in row_sends[k]:
            copy.start()

    ahead = min(3, chunks)
    routing_arrived(2)
    weights = gate_matrix(2)
    rows_arrived(2, 0)
    start_rows(1)
    partial_sum(2, 0, weights)
    for t in range(ahead):
        send(0, t)
    rows_arrived(2, 1)
    start_rows(3)
    partial_sum(2, 1, weights)
    for t in range(ahead):
        send(1, t)
    for i in range(ksteps):
        for copy in load_gate_up(i):
            copy.start()
    routing_arrived(1)
    weights = gate_matrix(1)
    rows_arrived(1, 0)
    rows_arrived(1, 1)
    start_rows(0)
    for h in range(2):
        partial_sum(1, h, weights)
    send(2, 0)
    routing_arrived(3)
    weights = gate_matrix(3)
    for h in range(2):
        rows_arrived(3, h)
        partial_sum(3, h, weights)
    send(3, 0)
    for n in range(2 * fsteps):
        load_rows(wd, n // fsteps, n % fsteps, 4 + n).start()

    def forward(t):
        tk = pl.ds(t * step_toks, step_toks)
        message(0, t).wait_recv()
        relay[0, tk, :] += part[1, tk, lo]
        send(4, t)
        message(1, t).wait_recv()
        relay[1, tk, :] += part[3, tk, hi]
        send(5, t)
        send(2, t + 1)
        send(3, t + 1)
        send(0, t + ahead)
        send(1, t + ahead)

    forward(0)

    for i in range(ksteps):
        for copy in load_gate_up(i):
            copy.wait()
        product = jnp.dot(normed[:, i * depth:(i + 1) * depth], pool[first_shared + i].reshape(depth, half), preferred_element_type=F32)
        part[0, :, lo] = product if i == 0 else part[0, :, lo] + product
    gate_act = part[0, :, pl.ds(0, ff)]
    hidden[...] = (gate_act * jax.nn.sigmoid(gate_act) * part[0, :, pl.ds(ff, ff)]).astype(BF16)
    weights = gate_matrix(0)
    for h in range(2):
        rows_arrived(0, h)
        partial_sum(0, h, weights)
    if chunks > 1:
        forward(1)
    for hh in range(2):
        for i in range(fsteps):
            load_rows(wd, hh, i, 4 + hh * fsteps + i).wait()
        for n in range(half // ncol):
            at = pl.ds(hh * half + n * ncol, ncol)
            product = None
            for i in range(fsteps):
                block = pool[4 + hh * fsteps + i, :, :, pl.ds(n * ncol, ncol)].reshape(depth, ncol)
                term = jnp.dot(hidden[:, i * depth:(i + 1) * depth], block, preferred_element_type=F32)
                product = term if product is None else product + term
            part[0, :, at] += resid[:, at].astype(F32) + product.astype(BF16).astype(F32)

    def shift(t):
        tk = pl.ds(t * step_toks, step_toks)
        return remote(ysend.at[tk], yin.at[tk], s_y.at[t], r_y.at[t], {"pp": nxt})

    def finish(t):
        tk = pl.ds(t * step_toks, step_toks)
        for kind in (2, 3, 4, 5):
            message(kind, t).wait_recv()
        ysend[tk, :] = (part[0, tk, :] + final[0, tk, :] + final[1, tk, :]).astype(BF16)
        shift(t).start()

    def receive(t):
        shift(t).wait_recv()
        for i in range(step_toks // blk):
            norm_rows(yin, gain_attn, t * (step_toks // blk) + i)

    for slot in range(nat_slots):
        load_heads(wq, slot, slot).start()

    def lay_out(j, carry):
        slot = lax.rem(j, nat_slots)
        load_heads(wq, j, slot).wait()
        pool.at[j][...] = nat.at[slot][...].reshape(groups, cap, half)

        @pl.when(j + nat_slots < slabs)
        def _():
            load_heads(wq, j + nat_slots, slot).start()

        @pl.when(j + nat_slots >= slabs)
        def _():
            load_heads(wk, j + nat_slots - slabs, slot).start()
        return carry

    per_chunk = -(-slabs // max(1, chunks - 2))
    done = 0
    for t in range(chunks):
        if t > 1:
            forward(t)
        if t > 0:
            finish(t - 1)
        if t > 1:
            receive(t - 2)
        upto = min(slabs, done + per_chunk) if t < chunks - 1 else slabs
        if upto > done:
            lax.fori_loop(done, upto, lay_out, 0)
        done = upto
    if chunks > 1:
        receive(chunks - 2)
    finish(chunks - 1)
    for t in range(chunks):
        for kind in range(6):
            message(kind, t).wait_send()
    part[1] = jnp.zeros((toks, dim), F32)
    part[2] = jnp.zeros((toks, dim), F32)
    part[3] = jnp.zeros((toks, dim), F32)
    receive(chunks - 1)

    qbuf, vbuf = resid, ysend

    def query(i, carry):
        for hh in range(2):
            at = halves[hh]
            product = jnp.dot(normed[:, pl.ds(pl.multiple_of(i * depth, depth), depth)], pool[hh * ksteps + i].reshape(depth, half), preferred_element_type=F32)
            part[1, :, at] += product
        load_rows(wo, 0, i, i).start()
        return carry

    lax.fori_loop(0, ksteps, query, 0)
    qbuf[...] = part[1].astype(BF16)

    def slot_of(index):
        return lax.rem(index, nat_slots)

    def stream(which, matrix, following):
        for hh in range(2):
            at = halves[hh]

            def step(i, carry):
                j = hh * ksteps + i
                slot = slot_of(j + (1 + which) * slabs)
                load_heads(matrix, j, slot).wait()
                part[2 + which, :, at] += jnp.dot(normed[:, pl.ds(pl.multiple_of(i * depth, depth), depth)], nat.at[slot][...].reshape(depth, half), preferred_element_type=F32)
                nj = j + nat_slots

                @pl.when(nj < slabs)
                def _():
                    load_heads(matrix, nj, slot).start()

                if following is not None:
                    @pl.when(nj >= slabs)
                    def _():
                        load_heads(following, nj - slabs, slot).start()

                if which == 1 and hh == 1:
                    load_rows(wo, 1, i, ksteps + i).start()
                return carry

            lax.fori_loop(0, ksteps, step, 0)

    stream(0, wk, wv)
    kbuf[...] = part[2].astype(BF16)
    stream(1, wv, None)
    for t in range(chunks):
        shift(t).wait_send()
    vbuf[...] = part[3].astype(BF16)

    scale = 1.0 / math.sqrt(head_dim)
    causal = lax.broadcasted_iota(jnp.int32, (toks, toks), 0) >= lax.broadcasted_iota(jnp.int32, (toks, toks), 1)
    together = 4

    def heads(n, carry):
        cols = [pl.ds(pl.multiple_of((n * together + m) * head_dim, head_dim), head_dim) for m in range(together)]
        scores = [lax.dot_general(qbuf[:, at], kbuf[:, at], (((1,), (1,)), ((), ())), preferred_element_type=F32) for at in cols]
        scores = [jnp.where(causal, s * scale, -1e30) for s in scores]
        probs = [jnp.exp(s - jnp.max(s, axis=-1, keepdims=True)) for s in scores]
        sums = [jnp.sum(p, axis=-1, keepdims=True) for p in probs]
        mixed = [jnp.dot(p.astype(BF16), vbuf[:, at], preferred_element_type=F32) for p, at in zip(probs, cols)]
        for at, value, total in zip(cols, mixed, sums):
            qbuf[:, at] = (value / total).astype(BF16)
        return carry

    lax.fori_loop(0, dim // (head_dim * together), heads, 0)

    out_copies = []
    for hh in range(2):
        at = halves[hh]
        for i in range(ksteps):
            load_rows(wo, hh, i, hh * ksteps + i).wait()
        for n in range(half // ncol):
            cols = pl.ds(hh * half + n * ncol, ncol)

            def proj(i, total):
                block = pool[hh * ksteps + i, :, :, pl.ds(n * ncol, ncol)].reshape(depth, ncol)
                return total + jnp.dot(qbuf[:, pl.ds(pl.multiple_of(i * depth, depth), depth)], block, preferred_element_type=F32)

            total = jnp.zeros((toks, ncol), F32)
            for i in range(ksteps):
                total = proj(i, total)
            kbuf[:, cols] = (yin[:, cols].astype(F32) + total.astype(BF16).astype(F32)).astype(BF16)
        copy = pltpu.make_async_copy(kbuf.at[:, at], out_hbm.at[:, at], s_load.at[hh])
        copy.start()
        out_copies.append(copy)

    for slot, copy in routing:
        copy.wait_send()
    for k in order:
        for copy in row_sends[k]:
            copy.wait_send()
    for copy in out_copies:
        copy.wait()


def run_stage(stages, chips, eo, ids, slots, gates, resid, gain_moe, gain_attn, wg, wu, wd, wq, wk, wv, wo):
    local_experts, owners, cap, dim = eo.shape
    toks = resid.shape[0]
    heads, head_dim = wq.shape[1:]
    ff = wg.shape[1]
    groups = 2 * local_experts
    depth = groups * cap
    half = dim // 2
    chunks = 8
    nat_slots = 4
    top_k = ids.shape[0]
    pool_slots = max(2 * dim // depth, 2 * chips + dim // depth)
    any_spec = pl.BlockSpec(memory_space=pl.ANY)
    dma = pltpu.SemaphoreType.DMA
    scratch = [
        pltpu.VMEM((pool_slots, groups, cap, half), BF16),
        pltpu.VMEM((nat_slots, depth, heads // 2, head_dim), BF16),
        pltpu.VMEM((chips, toks, dim), F32),
        pltpu.VMEM((2, toks, half), F32),
        pltpu.VMEM((2, toks, dim), F32),
        pltpu.VMEM((chips, top_k, toks), jnp.int32),
        pltpu.VMEM((chips, top_k, toks), jnp.int32),
        pltpu.VMEM((chips, top_k, toks), F32),
        pltpu.VMEM((1, dim), F32),
        pltpu.VMEM((1, dim), F32),
        pltpu.VMEM((toks, dim), BF16),
        pltpu.VMEM((toks, dim), BF16),
        pltpu.VMEM((toks, ff), BF16),
        pltpu.VMEM((toks, dim), BF16),
        pltpu.VMEM((toks, dim), BF16),
        pltpu.VMEM((toks, dim), BF16),
        dma((2 * chips + 6,)), dma((2, pool_slots)), dma((nat_slots,)), dma((2 * chips,)), dma((2 * chips,)),
        dma((chips, 3)), dma((chips, 3)), dma((6, chunks)), dma((6, chunks)), dma((chunks,)), dma((chunks,)),
    ]

    def grouped(matrix):
        return matrix.reshape(-1, cap, matrix.shape[-1])

    return pl.pallas_call(
        functools.partial(stage_kernel, chunks, stages, chips),
        out_shape=jax.ShapeDtypeStruct((toks, dim), BF16),
        in_specs=[any_spec] * 14,
        out_specs=any_spec,
        scratch_shapes=scratch,
        cost_estimate=pl.CostEstimate(flops=40_000_000_000, bytes_accessed=180_000_000, transcendentals=0),
        compiler_params=pltpu.CompilerParams(collective_id=0, has_side_effects=True, vmem_limit_bytes=67_043_328),
        name="stage",
    )(eo, ids, slots, gates, resid, gain_moe, gain_attn, grouped(wg), grouped(wu), grouped(wd), wq, wk, wv, grouped(wo))


def solution(mesh):
    stages = mesh.shape["pp"]
    ep_size = mesh.shape["ep"]
    tok_spec = P("pp", "data", "ep", None, None)
    vec_spec = P("pp", None)
    mat_spec = P("pp", None, None)
    head_spec = P("pp", None, None, None)

    def device_step(expert_out, expert_ids, slot_ids, gate_weights, residual, norm_moe, w_gate, w_up, w_down, norm_attn, w_query, w_key, w_value, w_out):
        local_experts, slots_total, model_dim = expert_out.shape[2:]
        cap = slots_total // ep_size
        eo = expert_out[0, 0].reshape(local_experts, ep_size, cap, model_dim)
        toks = residual.shape[3]

        def flip(array):
            return jnp.swapaxes(array[0, 0].reshape(toks, -1), 0, 1)

        out = run_stage(stages, ep_size // 2, eo, flip(expert_ids), flip(slot_ids), flip(gate_weights), residual[0, 0, 0],
                        norm_moe, norm_attn, w_gate[0], w_up[0], w_down[0], w_query[0], w_key[0], w_value[0],
                        w_out[0].reshape(-1, model_dim))
        return out[None, None, None]

    in_specs = (tok_spec,) * 5 + (vec_spec, mat_spec, mat_spec, mat_spec, vec_spec, head_spec, head_spec, head_spec, head_spec)
    return jax.shard_map(device_step, mesh=mesh, in_specs=in_specs, out_specs=tok_spec, check_vma=False)
```

```python
import functools
import math
import jax
import jax.numpy as jnp
from jax import lax
from jax.experimental import pallas as pl
from jax.experimental.pallas import tpu as pltpu
from jax.sharding import PartitionSpec as P

EPSILON = 1e-6
BF16 = jnp.bfloat16
F32 = jnp.float32
MESH = pl.DeviceIdType.MESH


def remote(src, dst, send, recv, where):
    return pltpu.make_async_remote_copy(src_ref=src, dst_ref=dst, send_sem=send, recv_sem=recv, device_id=where, device_id_type=MESH)


def stage_kernel(nat_shape, chunks, stages, chips, *refs):
    pl.run_scoped(functools.partial(stage_body, chunks, stages, chips, refs), pltpu.VMEM(nat_shape, BF16))


def stage_body(chunks, stages, chips, refs, nat):
    (eo, ids, slots, gates, resid_hbm, gain_moe_hbm, gain_attn_hbm, wg, wu, wd, wq, wk, wv, wo, out_hbm, key_hbm,
        pool, part, relay, final, r_ids, r_slots, r_gates, gain_moe, gain_attn, resid, normed, hidden, ysend, yin, kbuf,
        s_load, s_pool, s_nat, s_back, s_rows, s_rowx, s_route, r_route, s_msg, r_msg, s_y, r_y) = refs
    toks, dim = resid.shape
    half = dim // 2
    groups = pool.shape[1]
    local_experts = groups // 2
    cap = pool.shape[2]
    depth = groups * cap
    step_toks = toks // chunks
    head_dim = nat.shape[3]
    half_heads = nat.shape[2]
    ksteps = dim // depth
    slabs = 2 * ksteps
    ff = wg.shape[2]
    fsteps = ff // depth
    nat_slots = nat.shape[0]
    me = lax.axis_index("ep")
    stage = lax.axis_index("pp")
    chip, core = lax.div(me, 2), lax.rem(me, 2)
    other = 1 - core

    def at_chip(offset, core_idx):
        return 2 * lax.rem(chip + offset, chips) + core_idx

    right, left, across, partner = at_chip(1, core), at_chip(chips - 1, core), at_chip(2, core), at_chip(0, other)
    nxt, prv = lax.rem(stage + 1, stages), lax.rem(stage + stages - 1, stages)
    order = (2, 1, 3, 0)
    halves = (pl.ds(0, half), pl.ds(half, half))
    lo, hi = halves

    barrier = pltpu.get_barrier_semaphore()
    for peer in ({"ep": across}, {"ep": right}, {"ep": left}, {"ep": partner}, {"pp": nxt}, {"pp": prv}):
        pl.semaphore_signal(barrier, inc=1, device_id=peer, device_id_type=MESH)
    own_loads = {}
    for k in order:
        own_loads[k] = [pltpu.make_async_copy(eo.at[:, at_chip(k, core), :, halves[h]],
                                              pool.at[2 * k + h, pl.ds(core * local_experts, local_experts)], s_load.at[2 * k + h])
                        for h in range(2)]
    small = [(resid_hbm, resid), (gain_moe_hbm, gain_moe), (gain_attn_hbm, gain_attn),
             (ids, r_ids.at[0]), (slots, r_slots.at[0]), (gates, r_gates.at[0])]
    small_loads = [pltpu.make_async_copy(src, dst, s_load.at[2 * chips + n]) for n, (src, dst) in enumerate(small)]
    for copy in own_loads[2] + small_loads:
        copy.start()
    pl.semaphore_wait(barrier, 6)

    routing = []
    for offset in (2, 1, 3):
        slot = (chips - offset) % chips
        for n, (src, dst) in enumerate(((ids, r_ids), (slots, r_slots), (gates, r_gates))):
            copy = remote(src, dst.at[slot], s_route.at[offset, n], r_route.at[slot, n], {"ep": at_chip(offset, core)})
            copy.start()
            routing.append((slot, copy))
    row_sends = {}
    for k in order:
        row_sends[k] = [remote(eo.at[:, at_chip(k, other), :, halves[h]],
                               pool.at[2 * k + h, pl.ds(core * local_experts, local_experts)],
                               s_rows.at[2 * k + h], s_rowx.at[2 * k + h], {"ep": partner})
                        for h in range(2)]
    for copy in row_sends[2]:
        copy.start()
    for k in order[1:]:
        for copy in own_loads[k]:
            copy.start()

    first_shared = 2 * chips

    def load_gate_up(i):
        slot = first_shared + i
        at = pl.ds(i * groups, groups)
        return (pltpu.make_async_copy(wg.at[at], pool.at[slot, :, :, pl.ds(0, ff)], s_pool.at[0, slot]),
                pltpu.make_async_copy(wu.at[at], pool.at[slot, :, :, pl.ds(ff, ff)], s_pool.at[1, slot]))

    def load_rows(matrix, hh, i, slot):
        return pltpu.make_async_copy(matrix.at[pl.ds(i * groups, groups), :, pl.ds(pl.multiple_of(hh * half, half), half)],
                                     pool.at[slot], s_pool.at[0, slot])

    def load_heads(matrix, j, slot):
        hh, i = lax.div(j, ksteps), lax.rem(j, ksteps)
        return pltpu.make_async_copy(matrix.at[pl.ds(i * depth, depth), pl.ds(pl.multiple_of(hh * half_heads, half_heads), half_heads)],
                                     nat.at[slot], s_nat.at[slot])

    blk = min(16, step_toks)

    def norm_rows(src, gain, i):
        at = pl.ds(pl.multiple_of(i * blk, blk), blk)
        values = src[at, :].astype(F32)
        inv = lax.rsqrt(jnp.mean(values * values, axis=-1, keepdims=True) + EPSILON)
        normed[at, :] = (values * inv * gain[...]).astype(BF16)

    for copy in small_loads:
        copy.wait()

    def norm_resid(i, carry):
        norm_rows(resid, gain_moe, i)
        return carry

    lax.fori_loop(0, toks // blk, norm_resid, 0)

    ncol = min(512, half)

    def gate_matrix(k):
        dst = at_chip(k, core)
        e, s, g = r_ids[k], r_slots[k], r_gates[k]
        where_row = jnp.where(s >= 0, (e - chip * (2 * local_experts)) * cap + s - dst * cap, -1)
        row_iota = lax.broadcasted_iota(jnp.int32, (depth, toks), 0)
        weight = jnp.zeros((depth, toks), F32)
        for j in range(e.shape[0]):
            weight = jnp.where(row_iota == where_row[j:j + 1, :], g[j:j + 1, :], weight)
        weight = weight.T
        high = weight.astype(BF16)
        rest = weight - high.astype(F32)
        mid = rest.astype(BF16)
        low = (rest - mid.astype(F32)).astype(BF16)
        return high, mid, low

    def partial_sum(k, h, weights):
        def column(n, carry):
            start = pl.multiple_of(n * ncol, ncol)
            block = pool[2 * k + h, :, :, pl.ds(start, ncol)].reshape(depth, ncol)
            total = jnp.dot(weights[0], block, preferred_element_type=F32)
            total += jnp.dot(weights[1], block, preferred_element_type=F32)
            total += jnp.dot(weights[2], block, preferred_element_type=F32)
            part[k, :, pl.ds(pl.multiple_of(h * half + start, ncol), ncol)] = total
            return carry

        lax.fori_loop(0, half // ncol, column, 0)

    def message(kind, t):
        tk = pl.ds(t * step_toks, step_toks)
        src, dst, dev = {
            0: (part.at[2, tk, lo], relay.at[0, tk], right),
            1: (part.at[2, tk, hi], relay.at[1, tk], left),
            2: (part.at[1, tk, hi], final.at[0, tk, hi], right),
            3: (part.at[3, tk, lo], final.at[1, tk, lo], left),
            4: (relay.at[0, tk], final.at[0, tk, lo], right),
            5: (relay.at[1, tk], final.at[1, tk, hi], left),
        }[kind]
        return remote(src, dst, s_msg.at[kind, t], r_msg.at[kind, t], {"ep": dev})

    def send(kind, t):
        if t < chunks:
            message(kind, t).start()

    def routing_arrived(k):
        for slot, copy in routing:
            if slot == k:
                copy.wait_recv()

    def rows_arrived(k, h):
        own_loads[k][h].wait()
        row_sends[k][h].wait_recv()

    def start_rows(k):
        for copy in row_sends[k]:
            copy.start()

    ahead = min(5, chunks)
    routing_arrived(2)
    weights = gate_matrix(2)
    rows_arrived(2, 0)
    start_rows(1)
    partial_sum(2, 0, weights)
    for t in range(ahead):
        send(0, t)
    rows_arrived(2, 1)
    start_rows(3)
    partial_sum(2, 1, weights)
    for t in range(ahead):
        send(1, t)
    for i in range(ksteps):
        for copy in load_gate_up(i):
            copy.start()
    routing_arrived(1)
    weights = gate_matrix(1)
    rows_arrived(1, 0)
    rows_arrived(1, 1)
    start_rows(0)
    for h in range(2):
        partial_sum(1, h, weights)
    send(2, 0)
    routing_arrived(3)
    weights = gate_matrix(3)
    for h in range(2):
        rows_arrived(3, h)
        partial_sum(3, h, weights)
    send(3, 0)
    for n in range(2 * fsteps):
        load_rows(wd, n // fsteps, n % fsteps, 4 + n).start()

    def forward(t):
        tk = pl.ds(t * step_toks, step_toks)
        message(0, t).wait_recv()
        relay[0, tk, :] += part[1, tk, lo]
        send(4, t)
        message(1, t).wait_recv()
        relay[1, tk, :] += part[3, tk, hi]
        send(5, t)
        send(2, t + 1)
        send(3, t + 1)
        send(0, t + ahead)
        send(1, t + ahead)

    forward(0)

    for i in range(ksteps):
        for copy in load_gate_up(i):
            copy.wait()
        product = jnp.dot(normed[:, i * depth:(i + 1) * depth], pool[first_shared + i].reshape(depth, half), preferred_element_type=F32)
        part[0, :, lo] = product if i == 0 else part[0, :, lo] + product
    gate_act = part[0, :, pl.ds(0, ff)]
    hidden[...] = (gate_act * jax.nn.sigmoid(gate_act) * part[0, :, pl.ds(ff, ff)]).astype(BF16)
    weights = gate_matrix(0)
    for h in range(2):
        rows_arrived(0, h)
        partial_sum(0, h, weights)
    if chunks > 1:
        forward(1)
    for hh in range(2):
        for i in range(fsteps):
            load_rows(wd, hh, i, 4 + hh * fsteps + i).wait()
        for n in range(half // ncol):
            at = pl.ds(hh * half + n * ncol, ncol)
            product = None
            for i in range(fsteps):
                block = pool[4 + hh * fsteps + i, :, :, pl.ds(n * ncol, ncol)].reshape(depth, ncol)
                term = jnp.dot(hidden[:, i * depth:(i + 1) * depth], block, preferred_element_type=F32)
                product = term if product is None else product + term
            part[0, :, at] += resid[:, at].astype(F32) + product.astype(BF16).astype(F32)

    def shift(t):
        tk = pl.ds(t * step_toks, step_toks)
        return remote(ysend.at[tk], yin.at[tk], s_y.at[t], r_y.at[t], {"pp": nxt})

    def finish(t):
        tk = pl.ds(t * step_toks, step_toks)
        for kind in (2, 3, 4, 5):
            message(kind, t).wait_recv()
        ysend[tk, :] = (part[0, tk, :] + final[0, tk, :] + final[1, tk, :]).astype(BF16)
        shift(t).start()

    def receive(t):
        shift(t).wait_recv()
        for i in range(step_toks // blk):
            norm_rows(yin, gain_attn, t * (step_toks // blk) + i)

    sources = (wk, wq, wv)

    def back(j):
        return pltpu.make_async_copy(pool.at[j], key_hbm.at[j], s_back.at[j])

    for slot in range(nat_slots):
        load_heads(wk, slot, slot).start()

    def next_load(which, j, slot):
        nj = j + nat_slots

        @pl.when(nj < slabs)
        def _():
            load_heads(sources[which], nj, slot).start()

        if which + 1 < len(sources):
            @pl.when(nj >= slabs)
            def _():
                load_heads(sources[which + 1], nj - slabs, slot).start()

    def lay_out(which, begin, end):
        def step(j, carry):
            slot = lax.rem(j + which * slabs, nat_slots)
            load_heads(sources[which], j, slot).wait()
            if which == 1:
                back(j).wait()
            pool.at[j][...] = nat.at[slot][...].reshape(groups, cap, half)
            if which == 0:
                back(j).start()
            next_load(which, j, slot)
            return carry

        if end > begin:
            lax.fori_loop(begin, end, step, 0)

    per_chunk = -(-2 * slabs // max(1, chunks - 3))
    done = 0
    for t in range(chunks):
        if t > 1:
            forward(t)
        if t > 0:
            finish(t - 1)
        if t > 1:
            receive(t - 2)
        if t > 1 or chunks < 4:
            upto = min(2 * slabs, done + per_chunk) if t < chunks - 1 else 2 * slabs
            lay_out(0, done, min(upto, slabs))
            lay_out(1, max(done, slabs) - slabs, upto - slabs)
            done = upto
    if chunks > 1:
        receive(chunks - 2)
    finish(chunks - 1)
    for t in range(chunks):
        for kind in range(6):
            message(kind, t).wait_send()
    part[1] = jnp.zeros((toks, dim), F32)
    part[2] = jnp.zeros((toks, dim), F32)
    part[3] = jnp.zeros((toks, dim), F32)
    receive(chunks - 1)

    qbuf, vbuf = resid, ysend

    def load_key(s_idx):
        return pltpu.make_async_copy(key_hbm.at[s_idx], pool.at[s_idx], s_pool.at[0, s_idx])

    def inputs(i):
        return normed[:, pl.ds(pl.multiple_of(i * depth, depth), depth)]

    def query(i, carry):
        for hh in range(2):
            part[1, :, halves[hh]] += jnp.dot(inputs(i), pool[hh * ksteps + i].reshape(depth, half), preferred_element_type=F32)
        load_key(i).start()
        return carry

    lax.fori_loop(0, ksteps, query, 0)
    qbuf[...] = part[1].astype(BF16)

    for hh in range(2):
        def value(i, carry):
            j = hh * ksteps + i
            slot = lax.rem(j + 2 * slabs, nat_slots)
            load_heads(wv, j, slot).wait()
            part[3, :, halves[hh]] += jnp.dot(inputs(i), nat.at[slot][...].reshape(depth, half), preferred_element_type=F32)
            next_load(2, j, slot)

            @pl.when(lax.rem(j, 2) == 1)
            def _():
                load_key(ksteps + lax.div(j, 2)).start()
            return carry

        lax.fori_loop(0, ksteps, value, 0)
    for t in range(chunks):
        shift(t).wait_send()
    vbuf[...] = part[3].astype(BF16)

    for hh in range(2):
        def key(i, carry):
            j = hh * ksteps + i
            load_key(j).wait()
            part[2, :, halves[hh]] += jnp.dot(inputs(i), pool[j].reshape(depth, half), preferred_element_type=F32)
            load_rows(wo, hh, i, j).start()
            return carry

        lax.fori_loop(0, ksteps, key, 0)
    kbuf[...] = part[2].astype(BF16)

    scale = 1.0 / math.sqrt(head_dim)
    causal = lax.broadcasted_iota(jnp.int32, (toks, toks), 0) >= lax.broadcasted_iota(jnp.int32, (toks, toks), 1)
    together = 4

    def heads(n, carry):
        cols = [pl.ds(pl.multiple_of((n * together + m) * head_dim, head_dim), head_dim) for m in range(together)]
        scores = [lax.dot_general(qbuf[:, at], kbuf[:, at], (((1,), (1,)), ((), ())), preferred_element_type=F32) for at in cols]
        scores = [jnp.where(causal, s * scale, -1e30) for s in scores]
        probs = [jnp.exp(s - jnp.max(s, axis=-1, keepdims=True)) for s in scores]
        sums = [jnp.sum(p, axis=-1, keepdims=True) for p in probs]
        mixed = [jnp.dot(p.astype(BF16), vbuf[:, at], preferred_element_type=F32) for p, at in zip(probs, cols)]
        for at, value, total in zip(cols, mixed, sums):
            qbuf[:, at] = (value / total).astype(BF16)
        return carry

    lax.fori_loop(0, dim // (head_dim * together), heads, 0)

    out_copies = []
    for hh in range(2):
        at = halves[hh]
        for i in range(ksteps):
            load_rows(wo, hh, i, hh * ksteps + i).wait()
        for n in range(half // ncol):
            cols = pl.ds(hh * half + n * ncol, ncol)

            def proj(i, total):
                block = pool[hh * ksteps + i, :, :, pl.ds(n * ncol, ncol)].reshape(depth, ncol)
                return total + jnp.dot(qbuf[:, pl.ds(pl.multiple_of(i * depth, depth), depth)], block, preferred_element_type=F32)

            total = jnp.zeros((toks, ncol), F32)
            for i in range(ksteps):
                total = proj(i, total)
            kbuf[:, cols] = (yin[:, cols].astype(F32) + total.astype(BF16).astype(F32)).astype(BF16)
        copy = pltpu.make_async_copy(kbuf.at[:, at], out_hbm.at[:, at], s_load.at[hh])
        copy.start()
        out_copies.append(copy)

    for slot, copy in routing:
        copy.wait_send()
    for k in order:
        for copy in row_sends[k]:
            copy.wait_send()
    for copy in out_copies:
        copy.wait()


def run_stage(stages, chips, eo, ids, slots, gates, resid, gain_moe, gain_attn, wg, wu, wd, wq, wk, wv, wo):
    local_experts, owners, cap, dim = eo.shape
    toks = resid.shape[0]
    heads, head_dim = wq.shape[1:]
    ff = wg.shape[1]
    groups = 2 * local_experts
    depth = groups * cap
    half = dim // 2
    chunks = 8
    nat_slots = 4
    top_k = ids.shape[0]
    pool_slots = max(2 * dim // depth, 2 * chips + dim // depth)
    any_spec = pl.BlockSpec(memory_space=pl.ANY)
    dma = pltpu.SemaphoreType.DMA
    scratch = [
        pltpu.VMEM((pool_slots, groups, cap, half), BF16),
        pltpu.VMEM((chips, toks, dim), F32),
        pltpu.VMEM((2, toks, half), F32),
        pltpu.VMEM((2, toks, dim), F32),
        pltpu.VMEM((chips, top_k, toks), jnp.int32),
        pltpu.VMEM((chips, top_k, toks), jnp.int32),
        pltpu.VMEM((chips, top_k, toks), F32),
        pltpu.VMEM((1, dim), F32),
        pltpu.VMEM((1, dim), F32),
        pltpu.VMEM((toks, dim), BF16),
        pltpu.VMEM((toks, dim), BF16),
        pltpu.VMEM((toks, ff), BF16),
        pltpu.VMEM((toks, dim), BF16),
        pltpu.VMEM((toks, dim), BF16),
        pltpu.VMEM((toks, dim), BF16),
        dma((2 * chips + 6,)), dma((2, pool_slots)), dma((nat_slots,)), dma((pool_slots,)), dma((2 * chips,)), dma((2 * chips,)),
        dma((chips, 3)), dma((chips, 3)), dma((6, chunks)), dma((6, chunks)), dma((chunks,)), dma((chunks,)),
    ]

    def grouped(matrix):
        return matrix.reshape(-1, cap, matrix.shape[-1])

    return pl.pallas_call(
        functools.partial(stage_kernel, (nat_slots, depth, heads // 2, head_dim), chunks, stages, chips),
        out_shape=(jax.ShapeDtypeStruct((toks, dim), BF16), jax.ShapeDtypeStruct((2 * dim // depth, groups, cap, half), BF16)),
        in_specs=[any_spec] * 14,
        out_specs=(any_spec, any_spec),
        scratch_shapes=scratch,
        cost_estimate=pl.CostEstimate(flops=40_000_000_000, bytes_accessed=180_000_000, transcendentals=0),
        compiler_params=pltpu.CompilerParams(collective_id=0, has_side_effects=True, vmem_limit_bytes=67_043_328),
        name="stage",
    )(eo, ids, slots, gates, resid, gain_moe, gain_attn, grouped(wg), grouped(wu), grouped(wd), wq, wk, wv, grouped(wo))[0]


def solution(mesh):
    stages = mesh.shape["pp"]
    ep_size = mesh.shape["ep"]
    tok_spec = P("pp", "data", "ep", None, None)
    vec_spec = P("pp", None)
    mat_spec = P("pp", None, None)
    head_spec = P("pp", None, None, None)

    def device_step(expert_out, expert_ids, slot_ids, gate_weights, residual, norm_moe, w_gate, w_up, w_down, norm_attn, w_query, w_key, w_value, w_out):
        local_experts, slots_total, model_dim = expert_out.shape[2:]
        cap = slots_total // ep_size
        eo = expert_out[0, 0].reshape(local_experts, ep_size, cap, model_dim)
        toks = residual.shape[3]

        def flip(array):
            return jnp.swapaxes(array[0, 0].reshape(toks, -1), 0, 1)

        out = run_stage(stages, ep_size // 2, eo, flip(expert_ids), flip(slot_ids), flip(gate_weights), residual[0, 0, 0],
                        norm_moe, norm_attn, w_gate[0], w_up[0], w_down[0], w_query[0], w_key[0], w_value[0],
                        w_out[0].reshape(-1, model_dim))
        return out[None, None, None]

    in_specs = (tok_spec,) * 5 + (vec_spec, mat_spec, mat_spec, mat_spec, vec_spec, head_spec, head_spec, head_spec, head_spec)
    return jax.shard_map(device_step, mesh=mesh, in_specs=in_specs, out_specs=tok_spec, check_vma=False)
```
